8 devices in a mesh: rep: 1 (over z), dp: 8 (over x, y, core).
Axes of the slice: x: 2, y: 2, z: 1, core: 2. Of those that a mesh axis runs over, the one named last changes fastest.
Arguments:
- x: bfloat16 [8, 2048, 1024], P(('rep', 'dp'))
- dy: bfloat16 [8, 2048, 1024], P(('rep', 'dp'))
- w_gate: bfloat16 [2, 1024, 3200], replicated
- w_up: bfloat16 [2, 1024, 3200], replicated
- w_down: bfloat16 [2, 3200, 1024], replicated
- m_w_gate: float32 [2, 1024, 3200], replicated
- m_w_up: float32 [2, 1024, 3200], replicated
- m_w_down: float32 [2, 3200, 1024], replicated
- v_w_gate: float32 [2, 1024, 3200], replicated
- v_w_up: float32 [2, 1024, 3200], replicated
- v_w_down: float32 [2, 3200, 1024], replicated
Outputs:
- output 1: bfloat16 [2, 1024, 3200], P('rep')
- output 2: bfloat16 [2, 1024, 3200], P('rep')
- output 3: bfloat16 [2, 3200, 1024], P('rep')
- output 4: float32 [2, 1024, 3200], P('rep')
- output 5: float32 [2, 1024, 3200], P('rep')
- output 6: float32 [2, 3200, 1024], P('rep')
- output 7: float32 [2, 1024, 3200], P('rep')
- output 8: float32 [2, 1024, 3200], P('rep')
- output 9: float32 [2, 3200, 1024], P('rep')
All inputs are finite; a program needn't handle non-finite values.
Results may differ from the reference program's by a relative error of at most 0.0225.
Values are sent between devices in bfloat16 or wider.
A program may use at most 2.75 GiB of HBM per device.

```python
import jax
import jax.numpy as jnp
from jax import lax

SEQUENCES = 8
TOKENS = 2048
D = 1024
FF = 3200
LAYERS = 2
NAMES = ("w_gate", "w_up", "w_down")
SHAPES = {"w_gate": (LAYERS, D, FF), "w_up": (LAYERS, D, FF), "w_down": (LAYERS, FF, D)}


def bump(key, n, height):
    away = (jnp.arange(n, dtype=jnp.int32) - jax.random.randint(key, (), 0, n, jnp.int32)) % n
    return jnp.where(away < n // 8, height, 1.0)


def together(key, own, strength):
    shared = jax.random.normal(key, own.shape[1:], jnp.float32)
    return (own + strength * shared) * lax.rsqrt(1 + strength * strength)


def setup_inputs(seed: int = 0, part: int = 0) -> dict:
    kx, kdy, ka, kb, kz, kf, kh, kl, *keys = jax.random.split(jax.random.key(seed), 8 + 3 * len(NAMES))
    kx, kdy, ka, kb = (jax.random.fold_in(k, part) for k in (kx, kdy, ka, kb))
    kw, km, kv = (keys[i::3] for i in range(3))
    shape = (SEQUENCES, TOKENS, D)
    much_x, much_dy = jax.random.uniform(kz, (2,), jnp.float32, 0.0, 1.0)
    loud = 2.0 ** jax.random.uniform(jax.random.fold_in(kz, 1), (), jnp.float32, -1.0, 2.0)
    layers = 2.0 ** jax.random.uniform(kl, (LAYERS, 1, 1), jnp.float32, -1.0, 1.0)
    x = together(ka, jax.random.normal(kx, shape, jnp.float32), much_x) * bump(kf, D, 4.0)
    dy = together(kb, jax.random.normal(kdy, shape, jnp.float32), much_dy)
    drawn = {"x": x.astype(jnp.bfloat16), "dy": (loud * dy * (SEQUENCES * TOKENS) ** -0.5).astype(jnp.bfloat16)}
    for key, name in zip(kw, NAMES, strict=True):
        w = jax.random.normal(key, SHAPES[name], jnp.float32) * SHAPES[name][1] ** -0.5
        drawn[name] = (w * {"w_gate": 1.0, "w_up": bump(kh, FF, 4.0), "w_down": layers}[name]).astype(jnp.bfloat16)
    for key, name in zip(km, NAMES, strict=True):
        drawn[f"m_{name}"] = 0.1 * jax.random.normal(key, SHAPES[name], jnp.float32)
    for key, name in zip(kv, NAMES, strict=True):
        drawn[f"v_{name}"] = jax.random.uniform(key, SHAPES[name], jnp.float32, 0.005, 0.015)
    return drawn


def matmul(a, w):
    return jnp.dot(a, w, preferred_element_type=jnp.float32).astype(jnp.bfloat16)


def normed(h):
    wide = h.astype(jnp.float32)
    scale = lax.rsqrt(jnp.mean(wide**2, -1, keepdims=True) + 1e-6)
    return (wide * scale).astype(jnp.bfloat16)


def layer(h, w):
    a = normed(h)
    gate = jnp.dot(a, w["w_gate"], preferred_element_type=jnp.float32)
    up = jnp.dot(a, w["w_up"], preferred_element_type=jnp.float32)
    return h + matmul((jax.nn.silu(gate) * up).astype(jnp.bfloat16), w["w_down"])


def adamw(w, m, v, g):
    m = 0.9 * m + 0.1 * g
    v = 0.95 * v + 0.05 * g * g
    step = m * lax.rsqrt(v + 1e-8) + 0.1 * w
    return (w - 0.02 * step).astype(jnp.bfloat16), m, v


def stack(weights, h):
    return lax.scan(lambda h, w: (layer(h, w), None), h, weights)[0]


def reference(x, dy, w_gate, w_up, w_down, m_w_gate, m_w_up, m_w_down, v_w_gate, v_w_up, v_w_down):
    weights = dict(zip(NAMES, (w_gate, w_up, w_down), strict=True))

    def take(so_far, sequence):
        h, by_y = sequence
        _, back = jax.vjp(lambda w: stack(w, h), weights)
        return jax.tree.map(lambda total, term: total + term.astype(jnp.float32), so_far, back(by_y)[0]), None

    none_yet = {name: jnp.zeros(w.shape, jnp.float32) for name, w in weights.items()}
    by_weights, _ = lax.scan(take, none_yet, (x, dy))
    gradients = [by_weights[name].astype(jnp.bfloat16).astype(jnp.float32) for name in NAMES]
    new = [
        adamw(w.astype(jnp.float32), m, v, g)
        for w, m, v, g in zip((w_gate, w_up, w_down), (m_w_gate, m_w_up, m_w_down), (v_w_gate, v_w_up, v_w_down), gradients, strict=True)
    ]
    return tuple(one[which] for which in range(3) for one in new)
```

```python
import functools

import jax
import jax.numpy as jnp
from jax import lax
from jax.experimental import pallas as pl
from jax.experimental.pallas import tpu as pltpu
from jax.sharding import PartitionSpec as P

NAMES = ("w_gate", "w_up", "w_down")
TOKENS, D, FF = 2048, 1024, 3200
BLOCK = 256
ROWS = 512
CHUNK = D // 8
VMEM = 66_000_000
NT = (((1,), (1,)), ((), ()))
F32, BF16 = jnp.float32, jnp.bfloat16


def dot(a, b):
    return jnp.dot(a, b, preferred_element_type=F32)


def dot_nt(a, b):
    return lax.dot_general(a, b, NT, preferred_element_type=F32)


def once(shape, index_map):
    return pl.BlockSpec(shape, index_map, pipeline_mode=pl.Buffered(1))


def rms(h):
    return lax.rsqrt(jnp.mean(h * h, -1, keepdims=True) + 1e-6)


def by_width(j, units, last, body):
    if last == BLOCK:
        pl.when(j < units)(lambda: body(BLOCK))
    else:
        pl.when(j < units - 1)(lambda: body(BLOCK))
        pl.when(j == units - 1)(lambda: body(last))


def forward_kernel(units, last, x_ref, wg_ref, wu_ref, wd_ref, gate_ref, up_ref, a_ref, h_ref, next_ref, acc):
    j = pl.program_id(0)

    @pl.when(j == 0)
    def _():
        @pl.loop(0, TOKENS // ROWS)
        def _(i):
            rows = pl.ds(pl.multiple_of(i * ROWS, ROWS), ROWS)
            wide = x_ref[rows, :].astype(F32)
            a_ref[rows, :] = (wide * rms(wide)).astype(BF16)
            acc[rows, :] = jnp.zeros((ROWS, D), F32)

    def body(width):
        @pl.loop(0, TOKENS // ROWS)
        def _(i):
            rows = pl.ds(pl.multiple_of(i * ROWS, ROWS), ROWS)
            a = a_ref[rows, :]
            gate = dot(a, wg_ref[:, :width])
            up = dot(a, wu_ref[:, :width])
            gate_ref[rows, :width] = gate
            up_ref[rows, :width] = up
            act = (gate * jax.nn.sigmoid(gate) * up).astype(BF16)
            acc[rows, :] += dot(act, wd_ref[:width, :])

    by_width(j, units, last, body)

    @pl.when(j == units - 1)
    def _():
        @pl.loop(0, TOKENS // ROWS)
        def _(i):
            rows = pl.ds(pl.multiple_of(i * ROWS, ROWS), ROWS)
            h = (x_ref[rows, :].astype(F32) + acc[rows, :].astype(BF16).astype(F32)).astype(BF16)
            h_ref[rows, :] = h
            wide = h.astype(F32)
            next_ref[rows, :] = (wide * rms(wide)).astype(BF16)


def forward(x, wg, wu, wd):
    units = pl.cdiv(FF, BLOCK)
    last = FF - (units - 1) * BLOCK
    whole = lambda j: (0, 0)
    return pl.pallas_call(
        functools.partial(forward_kernel, units, last),
        grid=(units,),
        in_specs=[
            once((TOKENS, D), whole),
            pl.BlockSpec((None, D, BLOCK), lambda j: (0, 0, j)),
            pl.BlockSpec((None, D, BLOCK), lambda j: (0, 0, j)),
            pl.BlockSpec((None, BLOCK, D), lambda j: (0, j, 0)),
        ],
        out_specs=[
            pl.BlockSpec((TOKENS, BLOCK), lambda j: (0, j)),
            pl.BlockSpec((TOKENS, BLOCK), lambda j: (0, j)),
            once((TOKENS, D), whole),
            once((TOKENS, D), whole),
            once((TOKENS, D), whole),
        ],
        out_shape=[jax.ShapeDtypeStruct((TOKENS, FF), F32)] * 2 + [jax.ShapeDtypeStruct((TOKENS, D), BF16)] * 3,
        scratch_shapes=[pltpu.VMEM((TOKENS, D), F32)],
        compiler_params=pltpu.CompilerParams(vmem_limit_bytes=VMEM),
        cost_estimate=pl.CostEstimate(flops=6 * TOKENS * D * FF, bytes_accessed=90_000_000, transcendentals=TOKENS * FF),
        name="forward0",
    )(x, wg, wu, wd)


def backward_kernel(units, last, inner, *refs):
    if inner:
        a_ref, dy_ref, wd_ref, gate_ref, up_ref, out_ref = refs[:6]
        rest = refs[6:]
    else:
        a_ref, dy_ref, wd_ref, wg_ref, wu_ref, out_ref, da_ref = refs[:7]
        rest = refs[7:]
    at, dyt, act_s, dg_s, du_s, stay, go, first, second, r_core, r_first, r_second = rest[:12]
    sems = rest[12:18]
    acc = None if inner else rest[18]
    core_send, core_recv, first_send, first_recv, second_send, second_recv = sems
    j = pl.program_id(0)
    me = lax.axis_index("dp")
    core, y, x = me % 2, (me // 2) % 2, me // 4
    partner = me + 1 - 2 * core
    along_x, along_y = me + 4 - 8 * x, me + 2 - 4 * y
    one = (1 - core) * along_x + core * along_y
    two = (1 - core) * along_y + core * along_x

    def copy_core(k):
        return pltpu.make_async_remote_copy(
            go.at[k % 2], r_core.at[k % 4], core_send.at[k], core_recv.at[k], device_id={"dp": partner}, device_id_type=pl.DeviceIdType.MESH
        )

    def copy_first(k):
        return pltpu.make_async_remote_copy(
            first.at[k % 2], r_first.at[k % 4], first_send.at[k], first_recv.at[k], device_id={"dp": one}, device_id_type=pl.DeviceIdType.MESH
        )

    def copy_second(k):
        return pltpu.make_async_remote_copy(
            second.at[k % 2], r_second.at[k % 4], second_send.at[k], second_recv.at[k], device_id={"dp": two}, device_id_type=pl.DeviceIdType.MESH
        )

    @pl.when(j == 0)
    def _():
        barrier = pltpu.get_barrier_semaphore()
        for other in (partner, along_x, along_y):
            pl.semaphore_signal(barrier, inc=1, device_id={"dp": other}, device_id_type=pl.DeviceIdType.MESH)
        pl.semaphore_wait(barrier, 3)
        for r in range(8):
            c, u, v = r // 4, (r // 2) % 2, r % 2
            owner_core = (core + c) % 2
            du, dv = (1 - owner_core) * u + owner_core * v, (1 - owner_core) * v + owner_core * u
            owner = ((x + du) % 2) * 4 + ((y + dv) % 2) * 2 + owner_core
            columns = pl.ds(pl.multiple_of(owner * CHUNK, CHUNK), CHUNK)
            at[r * CHUNK : (r + 1) * CHUNK, :] = a_ref[:, columns].T
            dyt[r * CHUNK : (r + 1) * CHUNK, :] = dy_ref[:, columns].T
        if not inner:
            acc[...] = jnp.zeros_like(acc)

    @pl.when(j >= 3)
    def _():
        k = j - 3
        copy_second(k).wait()
        s, r = k % 4, k % 4
        total = stay[s, 0].astype(F32) + r_core[r, 0].astype(F32) + r_first[r, 0].astype(F32) + r_second[r].astype(F32)
        out_ref[...] = total.astype(BF16)

    @pl.when((j >= 2) & (j < units + 2))
    def _():
        k = j - 2
        copy_first(k).wait()
        s = k % 4
        second[k % 2] = (stay[s, 1].astype(F32) + r_core[s, 1].astype(F32) + r_first[s, 1].astype(F32)).astype(BF16)
        copy_second(k).start()

    @pl.when((j >= 1) & (j < units + 1))
    def _():
        k = j - 1
        copy_core(k).wait()
        s = k % 4
        first[k % 2] = (stay[s, 2:].astype(F32) + r_core[s, 2:].astype(F32)).astype(BF16)
        copy_first(k).start()

    def body(width):
        @pl.loop(0, TOKENS // ROWS)
        def _(i):
            rows = pl.ds(pl.multiple_of(i * ROWS, ROWS), ROWS)
            if inner:
                gate, up = gate_ref[rows, :width], up_ref[rows, :width]
            else:
                a = a_ref[rows, :]
                gate = dot(a, wg_ref[:, :width])
                up = dot(a, wu_ref[:, :width])
            by_act = dot_nt(dy_ref[rows, :], wd_ref[:width, :]).astype(BF16).astype(F32)
            sig = jax.nn.sigmoid(gate)
            silu = gate * sig
            act_s[rows, :width] = (silu * up).astype(BF16)
            du = (by_act * silu).astype(BF16)
            dg = (by_act * up * (sig + silu * (1.0 - sig))).astype(BF16)
            dg_s[rows, :width] = dg
            du_s[rows, :width] = du
            if not inner:
                acc[rows, :] += dot_nt(dg, wg_ref[:, :width]) + dot_nt(du, wu_ref[:, :width])

        def gradients(c, into):
            half = pl.ds(c * 4 * CHUNK, 4 * CHUNK)
            for which, (left, right) in enumerate(((at, dg_s), (at, du_s), (dyt, act_s))):
                term = dot(left[half, :], right[:, :width]).astype(BF16)
                into[:, which, :, :width] = term.reshape(4, CHUNK, width)

        gradients(1, go.at[j % 2])
        copy_core(j).start()
        gradients(0, stay.at[j % 4])

    by_width(j, units, last, body)

    if not inner:

        @pl.when(j == units)
        def _():
            da_ref[...] = acc[...].astype(BF16)


def backward(layer, first, size, inner, collective_id, a, dy, wd, left, right):
    units = pl.cdiv(size, BLOCK)
    last = size - (units - 1) * BLOCK
    start = first // BLOCK
    whole = lambda j: (0, 0)
    unit = lambda j: start + jnp.minimum(j, units - 1)
    in_specs = [once((TOKENS, D), whole), once((TOKENS, D), whole), pl.BlockSpec((None, BLOCK, D), lambda j: (layer, unit(j), 0))]
    if inner:
        in_specs += [pl.BlockSpec((TOKENS, BLOCK), lambda j: (0, unit(j)))] * 2
    else:
        in_specs += [pl.BlockSpec((None, D, BLOCK), lambda j: (layer, 0, unit(j)))] * 2
    out_specs = [pl.BlockSpec((3, CHUNK, BLOCK), lambda j: (0, 0, jnp.clip(j - 3, 0, units - 1)))]
    out_shape = [jax.ShapeDtypeStruct((3, CHUNK, size), BF16)]
    scratch = [
        pltpu.VMEM((D, TOKENS), BF16),
        pltpu.VMEM((D, TOKENS), BF16),
        pltpu.VMEM((TOKENS, BLOCK), BF16),
        pltpu.VMEM((TOKENS, BLOCK), BF16),
        pltpu.VMEM((TOKENS, BLOCK), BF16),
        pltpu.VMEM((4, 4, 3, CHUNK, BLOCK), BF16),
        pltpu.VMEM((2, 4, 3, CHUNK, BLOCK), BF16),
        pltpu.VMEM((2, 2, 3, CHUNK, BLOCK), BF16),
        pltpu.VMEM((2, 3, CHUNK, BLOCK), BF16),
        pltpu.VMEM((4, 4, 3, CHUNK, BLOCK), BF16),
        pltpu.VMEM((4, 2, 3, CHUNK, BLOCK), BF16),
        pltpu.VMEM((4, 3, CHUNK, BLOCK), BF16),
    ] + [pltpu.SemaphoreType.DMA((units,))] * 6
    if not inner:
        out_specs.append(once((TOKENS, D), whole))
        out_shape.append(jax.ShapeDtypeStruct((TOKENS, D), BF16))
        scratch.append(pltpu.VMEM((TOKENS, D), F32))
    return pl.pallas_call(
        functools.partial(backward_kernel, units, last, inner),
        grid=(units + 3,),
        in_specs=in_specs,
        out_specs=out_specs,
        out_shape=out_shape,
        scratch_shapes=scratch,
        compiler_params=pltpu.CompilerParams(vmem_limit_bytes=VMEM, collective_id=collective_id, has_side_effects=True),
        cost_estimate=pl.CostEstimate(flops=(8 if inner else 16) * TOKENS * D * size, bytes_accessed=40_000_000, transcendentals=TOKENS * size),
        name=f"backward{layer}_{first}",
    )(a, dy, wd, left, right)


WIDE = 640


def adamw_kernel(g_ref, *refs):
    ins, outs = refs[:9], refs[-9:]
    for which in range(3):
        g = g_ref[which].astype(F32)
        if which == 2:
            g = g.T
        w, m, v = (ins[3 * kind + which][...].astype(F32) for kind in range(3))
        m = 0.9 * m + 0.1 * g
        v = 0.95 * v + 0.05 * g * g
        step = m * lax.rsqrt(v + 1e-8) + 0.1 * w
        outs[which][...] = (w - 0.02 * step).astype(BF16)
        outs[3 + which][...] = m
        outs[6 + which][...] = v


def adamw(layer, first, size, g, arrays, so_far):
    start = first // WIDE
    row = pl.BlockSpec((None, CHUNK, WIDE), lambda k, i: (layer, k, start + i))
    column = pl.BlockSpec((None, WIDE, CHUNK), lambda k, i: (layer, start + i, k))
    nine = [row, row, column] * 3
    in_specs = [pl.BlockSpec((None, 3, CHUNK, WIDE), lambda k, i: (k, 0, 0, i))] + nine
    aliases = {}
    if so_far:
        in_specs += [pl.BlockSpec(memory_space=pl.ANY)] * 9
        aliases = {10 + i: i for i in range(9)}
    types = [BF16] * 3 + [F32] * 6
    elements = 3 * D * size
    return pl.pallas_call(
        adamw_kernel,
        grid=(8, size // WIDE),
        in_specs=in_specs,
        out_specs=nine,
        out_shape=[jax.ShapeDtypeStruct(a.shape, t) for a, t in zip(arrays, types)],
        input_output_aliases=aliases,
        compiler_params=pltpu.CompilerParams(vmem_limit_bytes=VMEM),
        cost_estimate=pl.CostEstimate(flops=40 * elements, bytes_accessed=22 * elements, transcendentals=elements),
        name=f"adamw{layer}_{first}",
    )(g, *arrays, *so_far)


PIECES = ((0, 1280), (1280, 1920))


def solution(mesh):
    def step(x, dy, *arrays):
        wg, wu, wd = arrays[:3]
        x, dy = x[0], dy[0]
        gate, up, a0, h1, a1 = forward(x, wg, wu, wd)
        g1, da = backward(1, 0, FF, False, 0, a1, dy, wd, wg, wu)
        gathered = [(1, 0, FF, lax.all_gather(g1, "dp"))]
        h, d = h1.astype(F32), da.astype(F32)
        scale = rms(h)
        dh = d * scale - h * (scale**3 / D) * jnp.sum(d * h, -1, keepdims=True)
        dh1 = (dy.astype(F32) + dh.astype(BF16).astype(F32)).astype(BF16)
        own = None
        for number, (first, size) in enumerate(PIECES):
            (own,) = backward(0, first, size, True, 1 + number, a0, dh1, wd, gate, up)
            gathered.append((0, first, size, lax.all_gather(own, "dp")))
        outs = ()
        for layer, first, size, g in gathered:
            outs = adamw(layer, first, size, g, arrays, outs)
        return tuple(outs)

    return jax.shard_map(
        step,
        mesh=mesh,
        in_specs=(P(("rep", "dp"), None, None),) * 2 + (P(None, None, None),) * 9,
        out_specs=(P("rep", None, None),) * 9,
        check_vma=False,
    )
```

```python
import functools

import jax
import jax.numpy as jnp
from jax import lax
from jax.experimental import pallas as pl
from jax.experimental.pallas import tpu as pltpu
from jax.sharding import PartitionSpec as P

NAMES = ("w_gate", "w_up", "w_down")
TOKENS, D, FF = 2048, 1024, 3200
BLOCK = 256
ROWS = 1024
LAG = 2
STEPS = 2 * LAG + 1
SLOTS = STEPS + 1
CHUNK = D // 8
VMEM = 66_000_000
NT = (((1,), (1,)), ((), ()))
F32, BF16 = jnp.float32, jnp.bfloat16


def dot(a, b):
    return jnp.dot(a, b, preferred_element_type=F32)


def dot_nt(a, b):
    return lax.dot_general(a, b, NT, preferred_element_type=F32)


def once(shape, index_map):
    return pl.BlockSpec(shape, index_map, pipeline_mode=pl.Buffered(1))


def rms(h):
    return lax.rsqrt(jnp.mean(h * h, -1, keepdims=True) + 1e-6)


def by_width(j, units, last, body):
    if last == BLOCK:
        pl.when(j < units)(lambda: body(BLOCK))
    else:
        pl.when(j < units - 1)(lambda: body(BLOCK))
        pl.when(j == units - 1)(lambda: body(last))


def forward_kernel(units, last, x_ref, wg_ref, wu_ref, wd_ref, gate_ref, up_ref, a_ref, h_ref, next_ref, acc):
    j = pl.program_id(0)

    @pl.when(j == 0)
    def _():
        for i in range(TOKENS // ROWS):
            rows = slice(i * ROWS, (i + 1) * ROWS)
            wide = x_ref[rows, :].astype(F32)
            a_ref[rows, :] = (wide * rms(wide)).astype(BF16)
            acc[rows, :] = jnp.zeros((ROWS, D), F32)

    def body(width):
        for i in range(TOKENS // ROWS):
            rows = slice(i * ROWS, (i + 1) * ROWS)
            a = a_ref[rows, :]
            gate = dot(a, wg_ref[:, :width])
            up = dot(a, wu_ref[:, :width])
            gate_ref[rows, :width] = gate
            up_ref[rows, :width] = up
            act = (gate * jax.nn.sigmoid(gate) * up).astype(BF16)
            acc[rows, :] += dot(act, wd_ref[:width, :])

    by_width(j, units, last, body)

    @pl.when(j == units - 1)
    def _():
        for i in range(TOKENS // ROWS):
            rows = slice(i * ROWS, (i + 1) * ROWS)
            h = (x_ref[rows, :].astype(F32) + acc[rows, :].astype(BF16).astype(F32)).astype(BF16)
            h_ref[rows, :] = h
            wide = h.astype(F32)
            next_ref[rows, :] = (wide * rms(wide)).astype(BF16)


def forward(x, wg, wu, wd):
    units = pl.cdiv(FF, BLOCK)
    last = FF - (units - 1) * BLOCK
    whole = lambda j: (0, 0)
    return pl.pallas_call(
        functools.partial(forward_kernel, units, last),
        grid=(units,),
        in_specs=[
            once((TOKENS, D), whole),
            pl.BlockSpec((None, D, BLOCK), lambda j: (0, 0, j)),
            pl.BlockSpec((None, D, BLOCK), lambda j: (0, 0, j)),
            pl.BlockSpec((None, BLOCK, D), lambda j: (0, j, 0)),
        ],
        out_specs=[
            pl.BlockSpec((TOKENS, BLOCK), lambda j: (0, j)),
            pl.BlockSpec((TOKENS, BLOCK), lambda j: (0, j)),
            once((TOKENS, D), whole),
            once((TOKENS, D), whole),
            once((TOKENS, D), whole),
        ],
        out_shape=[jax.ShapeDtypeStruct((TOKENS, FF), F32)] * 2 + [jax.ShapeDtypeStruct((TOKENS, D), BF16)] * 3,
        scratch_shapes=[pltpu.VMEM((TOKENS, D), F32)],
        compiler_params=pltpu.CompilerParams(vmem_limit_bytes=VMEM),
        cost_estimate=pl.CostEstimate(flops=6 * TOKENS * D * FF, bytes_accessed=90_000_000, transcendentals=TOKENS * FF),
        name="forward0",
    )(x, wg, wu, wd)


def backward_kernel(units, last, inner, *refs):
    if inner:
        a_ref, dy_ref, wd_ref, gate_ref, up_ref, out_ref = refs[:6]
        rest = refs[6:]
    else:
        a_ref, dy_ref, wd_ref, wg_ref, wu_ref, out_ref, dg_out, du_out = refs[:8]
        rest = refs[8:]
    at, dyt, act_s, dgu_s, stay, go, first, second, r_core, r_first, r_second = rest[:11]
    sems = rest[11:17]
    core_send, core_recv, first_send, first_recv, second_send, second_recv = sems
    j = pl.program_id(0)
    me = lax.axis_index("dp")
    core, y, x = me % 2, (me // 2) % 2, me // 4
    partner = me + 1 - 2 * core
    along_x, along_y = me + 4 - 8 * x, me + 2 - 4 * y
    one = (1 - core) * along_x + core * along_y
    two = (1 - core) * along_y + core * along_x

    def copy_core(k):
        return pltpu.make_async_remote_copy(
            go.at[k % 2], r_core.at[k % SLOTS], core_send.at[k], core_recv.at[k], device_id={"dp": partner}, device_id_type=pl.DeviceIdType.MESH
        )

    def copy_first(k):
        return pltpu.make_async_remote_copy(
            first.at[k % 2], r_first.at[k % SLOTS], first_send.at[k], first_recv.at[k], device_id={"dp": one}, device_id_type=pl.DeviceIdType.MESH
        )

    def copy_second(k):
        return pltpu.make_async_remote_copy(
            second.at[k % 2], r_second.at[k % SLOTS], second_send.at[k], second_recv.at[k], device_id={"dp": two}, device_id_type=pl.DeviceIdType.MESH
        )

    @pl.when(j == 0)
    def _():
        barrier = pltpu.get_barrier_semaphore()
        for other in (partner, along_x, along_y):
            pl.semaphore_signal(barrier, inc=1, device_id={"dp": other}, device_id_type=pl.DeviceIdType.MESH)
        pl.semaphore_wait(barrier, 3)
        for r in range(8):
            c, u, v = r // 4, (r // 2) % 2, r % 2
            owner_core = (core + c) % 2
            du, dv = (1 - owner_core) * u + owner_core * v, (1 - owner_core) * v + owner_core * u
            owner = ((x + du) % 2) * 4 + ((y + dv) % 2) * 2 + owner_core
            columns = pl.ds(pl.multiple_of(owner * CHUNK, CHUNK), CHUNK)
            at[r * CHUNK : (r + 1) * CHUNK, :] = a_ref[:, columns].T
            dyt[r * CHUNK : (r + 1) * CHUNK, :] = dy_ref[:, columns].T

    @pl.when(j >= STEPS)
    def _():
        k = j - STEPS
        copy_second(k).wait()
        s = k % SLOTS
        total = stay[s, 0].astype(F32) + r_core[s, 0].astype(F32) + r_first[s, 0].astype(F32) + r_second[s].astype(F32)
        out_ref[...] = total.astype(BF16)

    @pl.when((j >= LAG + 1) & (j < units + LAG + 1))
    def _():
        k = j - LAG - 1
        copy_first(k).wait()
        s = k % SLOTS
        second[k % 2] = (stay[s, 1].astype(F32) + r_core[s, 1].astype(F32) + r_first[s, 1].astype(F32)).astype(BF16)
        copy_second(k).start()

    @pl.when((j >= 1) & (j < units + 1))
    def _():
        k = j - 1
        copy_core(k).wait()
        s = k % SLOTS
        first[k % 2] = (stay[s, 2:].astype(F32) + r_core[s, 2:].astype(F32)).astype(BF16)
        copy_first(k).start()

    def body(width):
        for i in range(TOKENS // ROWS):
            rows = slice(i * ROWS, (i + 1) * ROWS)
            if inner:
                gate, up = gate_ref[rows, :width], up_ref[rows, :width]
            else:
                a = a_ref[rows, :]
                gate = dot(a, wg_ref[:, :width])
                up = dot(a, wu_ref[:, :width])
            by_act = dot_nt(dy_ref[rows, :], wd_ref[:width, :]).astype(BF16).astype(F32)
            sig = jax.nn.sigmoid(gate)
            silu = gate * sig
            act_s[rows, :width] = (silu * up).astype(BF16)
            du = (by_act * silu).astype(BF16)
            dg = (by_act * up * (sig + silu * (1.0 - sig))).astype(BF16)
            dgu_s[rows, :width] = dg
            dgu_s[rows, width : 2 * width] = du
            if not inner:
                dg_out[rows, :width] = dg
                du_out[rows, :width] = du

        def gradients(c, into):
            half = pl.ds(c * 4 * CHUNK, 4 * CHUNK)
            term = dot(at[half, :], dgu_s[:, : 2 * width]).astype(BF16)
            into[:, 0, :, :width] = term[:, :width].reshape(4, CHUNK, width)
            into[:, 1, :, :width] = term[:, width:].reshape(4, CHUNK, width)
            into[:, 2, :, :width] = dot(dyt[half, :], act_s[:, :width]).astype(BF16).reshape(4, CHUNK, width)

        gradients(1, go.at[j % 2])
        copy_core(j).start()
        gradients(0, stay.at[j % SLOTS])

    by_width(j, units, last, body)


def backward(layer, first, size, inner, collective_id, a, dy, wd, left, right):
    units = pl.cdiv(size, BLOCK)
    last = size - (units - 1) * BLOCK
    start = first // BLOCK
    whole = lambda j: (0, 0)
    unit = lambda j: start + jnp.minimum(j, units - 1)
    in_specs = [once((TOKENS, D), whole), once((TOKENS, D), whole), pl.BlockSpec((None, BLOCK, D), lambda j: (layer, unit(j), 0))]
    if inner:
        in_specs += [pl.BlockSpec((TOKENS, BLOCK), lambda j: (0, unit(j)))] * 2
    else:
        in_specs += [pl.BlockSpec((None, D, BLOCK), lambda j: (layer, 0, unit(j)))] * 2
    out_specs = [pl.BlockSpec((3, CHUNK, BLOCK), lambda j: (0, 0, jnp.clip(j - STEPS, 0, units - 1)))]
    out_shape = [jax.ShapeDtypeStruct((3, CHUNK, size), BF16)]
    scratch = [
        pltpu.VMEM((D, TOKENS), BF16),
        pltpu.VMEM((D, TOKENS), BF16),
        pltpu.VMEM((TOKENS, BLOCK), BF16),
        pltpu.VMEM((TOKENS, 2 * BLOCK), BF16),
        pltpu.VMEM((SLOTS, 4, 3, CHUNK, BLOCK), BF16),
        pltpu.VMEM((2, 4, 3, CHUNK, BLOCK), BF16),
        pltpu.VMEM((2, 2, 3, CHUNK, BLOCK), BF16),
        pltpu.VMEM((2, 3, CHUNK, BLOCK), BF16),
        pltpu.VMEM((SLOTS, 4, 3, CHUNK, BLOCK), BF16),
        pltpu.VMEM((SLOTS, 2, 3, CHUNK, BLOCK), BF16),
        pltpu.VMEM((SLOTS, 3, CHUNK, BLOCK), BF16),
    ] + [pltpu.SemaphoreType.DMA((units,))] * 6
    if not inner:
        out_specs += [pl.BlockSpec((TOKENS, BLOCK), lambda j: (0, jnp.minimum(j, units - 1)))] * 2
        out_shape += [jax.ShapeDtypeStruct((TOKENS, size), BF16)] * 2
    return pl.pallas_call(
        functools.partial(backward_kernel, units, last, inner),
        grid=(units + STEPS,),
        in_specs=in_specs,
        out_specs=out_specs,
        out_shape=out_shape,
        scratch_shapes=scratch,
        compiler_params=pltpu.CompilerParams(vmem_limit_bytes=VMEM, collective_id=collective_id, has_side_effects=True),
        cost_estimate=pl.CostEstimate(flops=(8 if inner else 12) * TOKENS * D * size, bytes_accessed=40_000_000, transcendentals=TOKENS * size),
        name=f"backward{layer}_{first}",
    )(a, dy, wd, left, right)


def input_kernel(pieces, *refs):
    grads, (wg_ref, wu_ref, h_ref, dy_ref, out_ref) = refs[: 2 * len(pieces)], refs[2 * len(pieces) :]
    da = None
    for number, (first, size) in enumerate(pieces):
        for g_ref, w_ref in zip(grads[2 * number : 2 * number + 2], (wg_ref, wu_ref)):
            part = dot_nt(g_ref[...], w_ref[:, first : first + size])
            da = part if da is None else da + part
    h, d = h_ref[...].astype(F32), da.astype(BF16).astype(F32)
    scale = rms(h)
    dh = d * scale - h * (scale**3 / D) * jnp.sum(d * h, -1, keepdims=True)
    out_ref[...] = (dy_ref[...].astype(F32) + dh.astype(BF16).astype(F32)).astype(BF16)


def by_input(layer, pieces, grads, wg, wu, h, dy):
    rows = 256
    weight = once((None, D, FF), lambda i: (layer, 0, 0))
    state = pl.BlockSpec((rows, D), lambda i: (i, 0))
    return pl.pallas_call(
        functools.partial(input_kernel, pieces),
        grid=(TOKENS // rows,),
        in_specs=[pl.BlockSpec((rows, size), lambda i: (i, 0)) for _, size in pieces for _ in range(2)] + [weight, weight, state, state],
        out_specs=state,
        out_shape=jax.ShapeDtypeStruct((TOKENS, D), BF16),
        compiler_params=pltpu.CompilerParams(vmem_limit_bytes=VMEM),
        cost_estimate=pl.CostEstimate(flops=4 * TOKENS * D * FF, bytes_accessed=50_000_000, transcendentals=TOKENS),
        name="by_input",
    )(*grads, wg, wu, h, dy)


WIDE = 640


def adamw_kernel(g_ref, *refs):
    ins, outs = refs[:9], refs[-9:]
    for which in range(3):
        g = g_ref[which].astype(F32)
        if which == 2:
            g = g.T
        w, m, v = (ins[3 * kind + which][...].astype(F32) for kind in range(3))
        m = 0.9 * m + 0.1 * g
        v = 0.95 * v + 0.05 * g * g
        step = m * lax.rsqrt(v + 1e-8) + 0.1 * w
        outs[which][...] = (w - 0.02 * step).astype(BF16)
        outs[3 + which][...] = m
        outs[6 + which][...] = v


def adamw(layer, first, size, g, arrays, so_far):
    start = first // WIDE
    row = pl.BlockSpec((None, CHUNK, WIDE), lambda k, i: (layer, k, start + i))
    column = pl.BlockSpec((None, WIDE, CHUNK), lambda k, i: (layer, start + i, k))
    nine = [row, row, column] * 3
    in_specs = [pl.BlockSpec((None, 3, CHUNK, WIDE), lambda k, i: (k, 0, 0, i))] + nine
    aliases = {}
    if so_far:
        in_specs += [pl.BlockSpec(memory_space=pl.ANY)] * 9
        aliases = {10 + i: i for i in range(9)}
    types = [BF16] * 3 + [F32] * 6
    elements = 3 * D * size
    return pl.pallas_call(
        adamw_kernel,
        grid=(8, size // WIDE),
        in_specs=in_specs,
        out_specs=nine,
        out_shape=[jax.ShapeDtypeStruct(a.shape, t) for a, t in zip(arrays, types)],
        input_output_aliases=aliases,
        compiler_params=pltpu.CompilerParams(vmem_limit_bytes=VMEM),
        cost_estimate=pl.CostEstimate(flops=40 * elements, bytes_accessed=22 * elements, transcendentals=elements),
        name=f"adamw{layer}_{first}",
    )(g, *arrays, *so_far)


PIECES = ((0, 1920), (1920, 1280))


def solution(mesh):
    def step(x, dy, *arrays):
        wg, wu, wd = arrays[:3]
        x, dy = x[0], dy[0]
        gate, up, a0, h1, a1 = forward(x, wg, wu, wd)
        own, *grads = backward(1, 0, FF, False, 0, a1, dy, wd, wg, wu)
        gathered = [(1, 0, FF, lax.all_gather(own, "dp"))]
        dh1 = by_input(1, ((0, FF),), grads, wg, wu, h1, dy)
        (own,) = backward(0, 0, FF, True, 1, a0, dh1, wd, gate, up)
        gathered += [(0, first, size, lax.all_gather(own[:, :, first : first + size], "dp")) for first, size in PIECES]
        outs = ()
        for layer, first, size, g in gathered:
            outs = adamw(layer, first, size, g, arrays, outs)
        return tuple(outs)

    return jax.shard_map(
        step,
        mesh=mesh,
        in_specs=(P(("rep", "dp"), None, None),) * 2 + (P(None, None, None),) * 9,
        out_specs=(P("rep", None, None),) * 9,
        check_vma=False,
    )
```

```python
import functools

import jax
import jax.numpy as jnp
from jax import lax
from jax.experimental import pallas as pl
from jax.experimental.pallas import tpu as pltpu
from jax.sharding import PartitionSpec as P

NAMES = ("w_gate", "w_up", "w_down")
TOKENS, D, FF = 2048, 1024, 3200
BLOCK = 256
ROWS = 1024
LAG = 2
STEPS = 2 * LAG + 1
SLOTS = STEPS + 1
SPLIT = 5
CHUNK = D // 8
VMEM = 66_000_000
NT = (((1,), (1,)), ((), ()))
F32, BF16 = jnp.float32, jnp.bfloat16


def dot(a, b):
    return jnp.dot(a, b, preferred_element_type=F32)


def dot_nt(a, b):
    return lax.dot_general(a, b, NT, preferred_element_type=F32)


def once(shape, index_map):
    return pl.BlockSpec(shape, index_map, pipeline_mode=pl.Buffered(1))


def rms(h):
    return lax.rsqrt(jnp.mean(h * h, -1, keepdims=True) + 1e-6)


def by_width(j, units, last, body):
    if last == BLOCK:
        pl.when(j < units)(lambda: body(BLOCK))
    else:
        pl.when(j < units - 1)(lambda: body(BLOCK))
        pl.when(j == units - 1)(lambda: body(last))


def forward_kernel(units, last, x_ref, wg_ref, wu_ref, wd_ref, gate_ref, up_ref, a_ref, h_ref, next_ref, acc):
    j = pl.program_id(0)

    @pl.when(j == 0)
    def _():
        for i in range(TOKENS // ROWS):
            rows = slice(i * ROWS, (i + 1) * ROWS)
            wide = x_ref[rows, :].astype(F32)
            a_ref[rows, :] = (wide * rms(wide)).astype(BF16)
            acc[rows, :] = jnp.zeros((ROWS, D), F32)

    def body(width):
        for i in range(TOKENS // ROWS):
            rows = slice(i * ROWS, (i + 1) * ROWS)
            a = a_ref[rows, :]
            gate = dot(a, wg_ref[:, :width])
            up = dot(a, wu_ref[:, :width])
            gate_ref[rows, :width] = gate
            up_ref[rows, :width] = up
            act = (gate * jax.nn.sigmoid(gate) * up).astype(BF16)
            acc[rows, :] += dot(act, wd_ref[:width, :])

    by_width(j, units, last, body)

    @pl.when(j == units - 1)
    def _():
        for i in range(TOKENS // ROWS):
            rows = slice(i * ROWS, (i + 1) * ROWS)
            h = (x_ref[rows, :].astype(F32) + acc[rows, :].astype(BF16).astype(F32)).astype(BF16)
            h_ref[rows, :] = h
            wide = h.astype(F32)
            next_ref[rows, :] = (wide * rms(wide)).astype(BF16)


def forward(x, wg, wu, wd):
    units = pl.cdiv(FF, BLOCK)
    last = FF - (units - 1) * BLOCK
    whole = lambda j: (0, 0)
    return pl.pallas_call(
        functools.partial(forward_kernel, units, last),
        grid=(units,),
        in_specs=[
            once((TOKENS, D), whole),
            pl.BlockSpec((None, D, BLOCK), lambda j: (0, 0, j)),
            pl.BlockSpec((None, D, BLOCK), lambda j: (0, 0, j)),
            pl.BlockSpec((None, BLOCK, D), lambda j: (0, j, 0)),
        ],
        out_specs=[
            pl.BlockSpec((TOKENS, BLOCK), lambda j: (0, j)),
            pl.BlockSpec((TOKENS, BLOCK), lambda j: (0, j)),
            once((TOKENS, D), whole),
            once((TOKENS, D), whole),
            once((TOKENS, D), whole),
        ],
        out_shape=[jax.ShapeDtypeStruct((TOKENS, FF), F32)] * 2 + [jax.ShapeDtypeStruct((TOKENS, D), BF16)] * 3,
        scratch_shapes=[pltpu.VMEM((TOKENS, D), F32)],
        compiler_params=pltpu.CompilerParams(vmem_limit_bytes=VMEM),
        cost_estimate=pl.CostEstimate(flops=6 * TOKENS * D * FF, bytes_accessed=90_000_000, transcendentals=TOKENS * FF),
        name="forward0",
    )(x, wg, wu, wd)


def backward_kernel(units, last, inner, *refs):
    if inner:
        a_ref, dy_ref, wd_ref, gate_ref, up_ref, early_ref, out_ref = refs[:7]
        rest = refs[7:]
    else:
        a_ref, dy_ref, wd_ref, wg_ref, wu_ref, early_ref, out_ref, dg_out, du_out = refs[:9]
        rest = refs[9:]
    at, dyt, act_s, dgu_s, stay, go, first, second, r_core, r_first, r_second = rest[:11]
    sems = rest[11:17]
    own, sent, got = (None, None, None) if inner else rest[17:20]
    core_send, core_recv, first_send, first_recv, second_send, second_recv = sems
    j = pl.program_id(0)
    me = lax.axis_index("dp")
    core, y, x = me % 2, (me // 2) % 2, me // 4
    partner = me + 1 - 2 * core
    along_x, along_y = me + 4 - 8 * x, me + 2 - 4 * y
    one = (1 - core) * along_x + core * along_y
    two = (1 - core) * along_y + core * along_x

    def copy_core(k):
        return pltpu.make_async_remote_copy(
            go.at[k % 2], r_core.at[k % SLOTS], core_send.at[k], core_recv.at[k], device_id={"dp": partner}, device_id_type=pl.DeviceIdType.MESH
        )

    def copy_first(k):
        return pltpu.make_async_remote_copy(
            first.at[k % 2], r_first.at[k % SLOTS], first_send.at[k], first_recv.at[k], device_id={"dp": one}, device_id_type=pl.DeviceIdType.MESH
        )

    def copy_second(k):
        return pltpu.make_async_remote_copy(
            second.at[k % 2], r_second.at[k % SLOTS], second_send.at[k], second_recv.at[k], device_id={"dp": two}, device_id_type=pl.DeviceIdType.MESH
        )

    @pl.when(j == 0)
    def _():
        barrier = pltpu.get_barrier_semaphore()
        for other in (partner, along_x, along_y):
            pl.semaphore_signal(barrier, inc=1, device_id={"dp": other}, device_id_type=pl.DeviceIdType.MESH)
        pl.semaphore_wait(barrier, 3)
        for r in range(8):
            c, u, v = r // 4, (r // 2) % 2, r % 2
            owner_core = (core + c) % 2
            du, dv = (1 - owner_core) * u + owner_core * v, (1 - owner_core) * v + owner_core * u
            owner = ((x + du) % 2) * 4 + ((y + dv) % 2) * 2 + owner_core
            columns = pl.ds(pl.multiple_of(owner * CHUNK, CHUNK), CHUNK)
            at[r * CHUNK : (r + 1) * CHUNK, :] = a_ref[:, columns].T
            dyt[r * CHUNK : (r + 1) * CHUNK, :] = dy_ref[:, columns].T

    def place(k, owner):
        return early_ref.at[owner, :, :, pl.ds(pl.multiple_of(k * BLOCK, BLOCK), BLOCK)]

    def keep(k):
        return pltpu.make_async_copy(own.at[k], place(k, me), sent.at[k, 7])

    def spread(k, way, source, owner, to):
        return pltpu.make_async_remote_copy(
            source, place(k, owner), sent.at[k, way], got.at[k, way], device_id={"dp": to}, device_id_type=pl.DeviceIdType.MESH
        )

    @pl.when(j >= STEPS)
    def _():
        k = j - STEPS
        copy_second(k).wait()
        s = k % SLOTS
        total = stay[s, 0].astype(F32) + r_core[s, 0].astype(F32) + r_first[s, 0].astype(F32) + r_second[s].astype(F32)
        if inner:

            @pl.when(k < SPLIT)
            def _():
                early_ref[...] = total.astype(BF16)

        @pl.when(k >= SPLIT)
        def _():
            out_ref[...] = total.astype(BF16)

        if not inner:

            @pl.when(k < SPLIT)
            def _():
                own[k] = total.astype(BF16)
                keep(k).start()
                for way, to in enumerate((two, one, partner)):
                    spread(k, way, own.at[k], me, to).start()

    if not inner:
        beyond = one + two - me

        @pl.when((j >= STEPS + LAG) & (j < STEPS + LAG + SPLIT))
        def _():
            k = j - STEPS - LAG
            spread(k, 0, own.at[k], me, two).wait_recv()
            spread(k, 3, place(k, two), two, one).start()
            spread(k, 4, place(k, two), two, partner).start()
            spread(k, 1, own.at[k], me, one).wait_recv()
            spread(k, 5, place(k, one), one, partner).start()

        @pl.when((j >= STEPS + 2 * LAG) & (j < STEPS + 2 * LAG + SPLIT))
        def _():
            k = j - STEPS - 2 * LAG
            spread(k, 3, place(k, two), two, one).wait_recv()
            spread(k, 6, place(k, beyond), beyond, partner).start()

        @pl.when((j >= STEPS + 3 * LAG) & (j < STEPS + 3 * LAG + SPLIT))
        def _():
            k = j - STEPS - 3 * LAG
            keep(k).wait()
            for way in range(7):
                spread(k, way, own.at[k], me, partner).wait_send()
            for way in (2, 4, 5, 6):
                spread(k, way, own.at[k], me, partner).wait_recv()

    @pl.when((j >= LAG + 1) & (j < units + LAG + 1))
    def _():
        k = j - LAG - 1
        copy_first(k).wait()
        s = k % SLOTS
        second[k % 2] = (stay[s, 1].astype(F32) + r_core[s, 1].astype(F32) + r_first[s, 1].astype(F32)).astype(BF16)
        copy_second(k).start()

    @pl.when((j >= 1) & (j < units + 1))
    def _():
        k = j - 1
        copy_core(k).wait()
        s = k % SLOTS
        first[k % 2] = (stay[s, 2:].astype(F32) + r_core[s, 2:].astype(F32)).astype(BF16)
        copy_first(k).start()

    def body(width):
        for i in range(TOKENS // ROWS):
            rows = slice(i * ROWS, (i + 1) * ROWS)
            if inner:
                gate, up = gate_ref[rows, :width], up_ref[rows, :width]
            else:
                a = a_ref[rows, :]
                gate = dot(a, wg_ref[:, :width])
                up = dot(a, wu_ref[:, :width])
            by_act = dot_nt(dy_ref[rows, :], wd_ref[:width, :]).astype(BF16).astype(F32)
            sig = jax.nn.sigmoid(gate)
            silu = gate * sig
            act_s[rows, :width] = (silu * up).astype(BF16)
            du = (by_act * silu).astype(BF16)
            dg = (by_act * up * (sig + silu * (1.0 - sig))).astype(BF16)
            dgu_s[rows, :width] = dg
            dgu_s[rows, width : 2 * width] = du
            if not inner:
                dg_out[rows, :width] = dg
                du_out[rows, :width] = du

        def gradients(c, into):
            half = pl.ds(c * 4 * CHUNK, 4 * CHUNK)
            term = dot(at[half, :], dgu_s[:, : 2 * width]).astype(BF16)
            into[:, 0, :, :width] = term[:, :width].reshape(4, CHUNK, width)
            into[:, 1, :, :width] = term[:, width:].reshape(4, CHUNK, width)
            into[:, 2, :, :width] = dot(dyt[half, :], act_s[:, :width]).astype(BF16).reshape(4, CHUNK, width)

        gradients(1, go.at[j % 2])
        copy_core(j).start()
        gradients(0, stay.at[j % SLOTS])

    by_width(j, units, last, body)


def backward(layer, inner, collective_id, a, dy, wd, left, right):
    units = pl.cdiv(FF, BLOCK)
    last = FF - (units - 1) * BLOCK
    size, early = FF, SPLIT * BLOCK
    assert units >= SPLIT + LAG + 1
    whole = lambda j: (0, 0)
    unit = lambda j: jnp.minimum(j, units - 1)
    in_specs = [once((TOKENS, D), whole), once((TOKENS, D), whole), pl.BlockSpec((None, BLOCK, D), lambda j: (layer, unit(j), 0))]
    if inner:
        in_specs += [pl.BlockSpec((TOKENS, BLOCK), lambda j: (0, unit(j)))] * 2
        out_specs = [pl.BlockSpec((3, CHUNK, BLOCK), lambda j: (0, 0, jnp.clip(j - STEPS, 0, SPLIT - 1)))]
        out_shape = [jax.ShapeDtypeStruct((3, CHUNK, early), BF16)]
    else:
        in_specs += [pl.BlockSpec((None, D, BLOCK), lambda j: (layer, 0, unit(j)))] * 2
        out_specs = [pl.BlockSpec(memory_space=pl.ANY)]
        out_shape = [jax.ShapeDtypeStruct((8, 3, CHUNK, early), BF16)]
    out_specs.append(pl.BlockSpec((3, CHUNK, BLOCK), lambda j: (0, 0, jnp.clip(j - STEPS - SPLIT, 0, units - SPLIT - 1))))
    out_shape.append(jax.ShapeDtypeStruct((3, CHUNK, FF - early), BF16))
    scratch = [
        pltpu.VMEM((D, TOKENS), BF16),
        pltpu.VMEM((D, TOKENS), BF16),
        pltpu.VMEM((TOKENS, BLOCK), BF16),
        pltpu.VMEM((TOKENS, 2 * BLOCK), BF16),
        pltpu.VMEM((SLOTS, 4, 3, CHUNK, BLOCK), BF16),
        pltpu.VMEM((2, 4, 3, CHUNK, BLOCK), BF16),
        pltpu.VMEM((2, 2, 3, CHUNK, BLOCK), BF16),
        pltpu.VMEM((2, 3, CHUNK, BLOCK), BF16),
        pltpu.VMEM((SLOTS, 4, 3, CHUNK, BLOCK), BF16),
        pltpu.VMEM((SLOTS, 2, 3, CHUNK, BLOCK), BF16),
        pltpu.VMEM((SLOTS, 3, CHUNK, BLOCK), BF16),
    ] + [pltpu.SemaphoreType.DMA((units,))] * 6
    if not inner:
        out_specs += [pl.BlockSpec((TOKENS, BLOCK), lambda j: (0, unit(j)))] * 2
        out_shape += [jax.ShapeDtypeStruct((TOKENS, size), BF16)] * 2
        scratch += [pltpu.VMEM((SPLIT, 3, CHUNK, BLOCK), BF16), pltpu.SemaphoreType.DMA((SPLIT, 8)), pltpu.SemaphoreType.DMA((SPLIT, 7))]
    return pl.pallas_call(
        functools.partial(backward_kernel, units, last, inner),
        grid=(units + STEPS,),
        in_specs=in_specs,
        out_specs=out_specs,
        out_shape=out_shape,
        scratch_shapes=scratch,
        compiler_params=pltpu.CompilerParams(vmem_limit_bytes=VMEM, collective_id=collective_id, has_side_effects=True),
        cost_estimate=pl.CostEstimate(flops=(8 if inner else 12) * TOKENS * D * size, bytes_accessed=40_000_000, transcendentals=TOKENS * size),
        name=f"backward{layer}",
    )(a, dy, wd, left, right)


def input_kernel(dg_ref, du_ref, wg_ref, wu_ref, h_ref, dy_ref, g_ref, *refs):
    out_ref = refs[9]
    da = dot_nt(dg_ref[...], wg_ref[...]) + dot_nt(du_ref[...], wu_ref[...])
    h, d = h_ref[...].astype(F32), da.astype(BF16).astype(F32)
    scale = rms(h)
    dh = d * scale - h * (scale**3 / D) * jnp.sum(d * h, -1, keepdims=True)
    out_ref[...] = (dy_ref[...].astype(F32) + dh.astype(BF16).astype(F32)).astype(BF16)
    adamw_kernel(g_ref, *refs[:9], *refs[10:])


def by_input(layer, dg, du, wg, wu, h, dy, g, arrays):
    rows = TOKENS // 8
    weight = once((None, D, FF), lambda i: (layer, 0, 0))
    state = pl.BlockSpec((rows, D), lambda i: (i, 0))
    more_in, more_out, more_shape = adamw_specs(layer, 0, SPLIT * BLOCK, SPLIT * BLOCK, arrays)
    elements = 3 * D * SPLIT * BLOCK
    return pl.pallas_call(
        input_kernel,
        grid=(8,),
        in_specs=[pl.BlockSpec((rows, FF), lambda i: (i, 0))] * 2 + [weight, weight, state, state] + more_in,
        out_specs=[state] + more_out,
        out_shape=[jax.ShapeDtypeStruct((TOKENS, D), BF16)] + more_shape,
        compiler_params=pltpu.CompilerParams(vmem_limit_bytes=VMEM),
        cost_estimate=pl.CostEstimate(flops=4 * TOKENS * D * FF, bytes_accessed=50_000_000 + 22 * elements, transcendentals=TOKENS + elements),
        name="by_input",
    )(dg, du, wg, wu, h, dy, g, *arrays)


WIDE = 640


def adamw_kernel(g_ref, *refs):
    ins, outs = refs[:9], refs[-9:]
    for which in range(3):
        g = g_ref[which].astype(F32)
        if which == 2:
            g = g.T
        w, m, v = (ins[3 * kind + which][...].astype(F32) for kind in range(3))
        m = 0.9 * m + 0.1 * g
        v = 0.95 * v + 0.05 * g * g
        step = m * lax.rsqrt(v + 1e-8) + 0.1 * w
        outs[which][...] = (w - 0.02 * step).astype(BF16)
        outs[3 + which][...] = m
        outs[6 + which][...] = v


def adamw_specs(layer, first, size, wide, arrays):
    start, across = first // wide, size // wide
    row = pl.BlockSpec((None, CHUNK, wide), lambda t: (layer, t // across, start + t % across))
    column = pl.BlockSpec((None, wide, CHUNK), lambda t: (layer, start + t % across, t // across))
    nine = [row, row, column] * 3
    types = [BF16] * 3 + [F32] * 6
    gradient = pl.BlockSpec((None, 3, CHUNK, wide), lambda t: (t // across, 0, 0, t % across))
    return [gradient] + nine, nine, [jax.ShapeDtypeStruct(a.shape, t) for a, t in zip(arrays, types)]


def adamw(layer, first, size, g, arrays, so_far):
    in_specs, out_specs, out_shape = adamw_specs(layer, first, size, WIDE, arrays)
    elements = 3 * D * size
    return pl.pallas_call(
        adamw_kernel,
        grid=(8 * size // WIDE,),
        in_specs=in_specs + [pl.BlockSpec(memory_space=pl.ANY)] * 9,
        out_specs=out_specs,
        out_shape=out_shape,
        input_output_aliases={10 + i: i for i in range(9)},
        compiler_params=pltpu.CompilerParams(vmem_limit_bytes=VMEM),
        cost_estimate=pl.CostEstimate(flops=40 * elements, bytes_accessed=22 * elements, transcendentals=elements),
        name=f"adamw{layer}_{first}",
    )(g, *arrays, *so_far)


def solution(mesh):
    def step(x, dy, *arrays):
        wg, wu, wd = arrays[:3]
        x, dy = x[0], dy[0]
        early = SPLIT * BLOCK
        gate, up, a0, h1, a1 = forward(x, wg, wu, wd)
        all1, own1, dg, du = backward(1, False, 0, a1, dy, wd, wg, wu)
        rest1 = lax.all_gather(own1, "dp")
        dh1, *outs = by_input(1, dg, du, wg, wu, h1, dy, all1, arrays)
        first0, own0 = backward(0, True, 1, a0, dh1, wd, gate, up)
        rest0 = lax.all_gather(own0, "dp")
        first0, _ = lax.optimization_barrier((first0, own0))
        first0 = lax.all_gather(first0, "dp")
        outs = adamw(1, early, FF - early, rest1, arrays, outs)
        outs = adamw(0, early, FF - early, rest0, arrays, outs)
        return tuple(adamw(0, 0, early, first0, arrays, outs))

    return jax.shard_map(
        step,
        mesh=mesh,
        in_specs=(P(("rep", "dp"), None, None),) * 2 + (P(None, None, None),) * 9,
        out_specs=(P("rep", None, None),) * 9,
        check_vma=False,
    )
```

```python
import functools

import jax
import jax.numpy as jnp
from jax import lax
from jax.experimental import pallas as pl
from jax.experimental.pallas import tpu as pltpu
from jax.sharding import PartitionSpec as P

NAMES = ("w_gate", "w_up", "w_down")
TOKENS, D, FF = 2048, 1024, 3200
BLOCK = 256
ROWS = 1024
FEW = 128
LAG = 2
STEPS = 2 * LAG + 1
SLOTS = STEPS + 1
SPLIT = 5
CHUNK = D // 8
VMEM = 66_000_000
NT = (((1,), (1,)), ((), ()))
F32, BF16 = jnp.float32, jnp.bfloat16


def dot(a, b):
    return jnp.dot(a, b, preferred_element_type=F32)


def dot_nt(a, b):
    return lax.dot_general(a, b, NT, preferred_element_type=F32)


def once(shape, index_map):
    return pl.BlockSpec(shape, index_map, pipeline_mode=pl.Buffered(1))


def rms(h):
    return lax.rsqrt(jnp.mean(h * h, -1, keepdims=True) + 1e-6)


def by_width(j, units, last, body):
    if last == BLOCK:
        pl.when(j < units)(lambda: body(BLOCK))
    else:
        pl.when(j < units - 1)(lambda: body(BLOCK))
        pl.when(j == units - 1)(lambda: body(last))


def forward_kernel(units, last, x_ref, wg_ref, wu_ref, wd_ref, gate_ref, up_ref, a_ref, h_ref, next_ref, acc):
    j = pl.program_id(0)

    @pl.when(j == 0)
    def _():
        @pl.loop(0, TOKENS // FEW)
        def _(i):
            rows = pl.ds(pl.multiple_of(i * FEW, FEW), FEW)
            wide = x_ref[rows, :].astype(F32)
            a_ref[rows, :] = (wide * rms(wide)).astype(BF16)
            acc[rows, :] = jnp.zeros((FEW, D), F32)

    def body(width):
        @pl.loop(0, TOKENS // ROWS)
        def _(i):
            rows = pl.ds(pl.multiple_of(i * ROWS, ROWS), ROWS)
            a = a_ref[rows, :]
            gate = dot(a, wg_ref[:, :width])
            up = dot(a, wu_ref[:, :width])
            gate_ref[rows, :width] = gate
            up_ref[rows, :width] = up
            act = (gate * jax.nn.sigmoid(gate) * up).astype(BF16)
            acc[rows, :] += dot(act, wd_ref[:width, :])

    by_width(j, units, last, body)

    @pl.when(j == units - 1)
    def _():
        @pl.loop(0, TOKENS // FEW)
        def _(i):
            rows = pl.ds(pl.multiple_of(i * FEW, FEW), FEW)
            h = (x_ref[rows, :].astype(F32) + acc[rows, :].astype(BF16).astype(F32)).astype(BF16)
            h_ref[rows, :] = h
            wide = h.astype(F32)
            next_ref[rows, :] = (wide * rms(wide)).astype(BF16)


def forward(x, wg, wu, wd):
    units = pl.cdiv(FF, BLOCK)
    last = FF - (units - 1) * BLOCK
    whole = lambda j: (0, 0)
    return pl.pallas_call(
        functools.partial(forward_kernel, units, last),
        grid=(units,),
        in_specs=[
            once((TOKENS, D), whole),
            pl.BlockSpec((None, D, BLOCK), lambda j: (0, 0, j)),
            pl.BlockSpec((None, D, BLOCK), lambda j: (0, 0, j)),
            pl.BlockSpec((None, BLOCK, D), lambda j: (0, j, 0)),
        ],
        out_specs=[
            pl.BlockSpec((TOKENS, BLOCK), lambda j: (0, j)),
            pl.BlockSpec((TOKENS, BLOCK), lambda j: (0, j)),
            once((TOKENS, D), whole),
            once((TOKENS, D), whole),
            once((TOKENS, D), whole),
        ],
        out_shape=[jax.ShapeDtypeStruct((TOKENS, FF), F32)] * 2 + [jax.ShapeDtypeStruct((TOKENS, D), BF16)] * 3,
        scratch_shapes=[pltpu.VMEM((TOKENS, D), F32)],
        compiler_params=pltpu.CompilerParams(vmem_limit_bytes=VMEM),
        cost_estimate=pl.CostEstimate(flops=6 * TOKENS * D * FF, bytes_accessed=90_000_000, transcendentals=TOKENS * FF),
        name="forward0",
    )(x, wg, wu, wd)


def backward_kernel(units, last, inner, *refs):
    if inner:
        a_ref, dy_ref, wd_ref, gate_ref, up_ref, early_ref, out_ref = refs[:7]
        rest = refs[7:]
    else:
        a_ref, dy_ref, wd_ref, wg_ref, wu_ref, early_ref, out_ref, dg_out, du_out = refs[:9]
        rest = refs[9:]
    at, dyt, act_s, dgu_s, stay, go, first, second, r_core, r_first, r_second = rest[:11]
    sems = rest[11:17]
    own, sent, got = (None, None, None) if inner else rest[17:20]
    core_send, core_recv, first_send, first_recv, second_send, second_recv = sems
    j = pl.program_id(0)
    me = lax.axis_index("dp")
    core, y, x = me % 2, (me // 2) % 2, me // 4
    partner = me + 1 - 2 * core
    along_x, along_y = me + 4 - 8 * x, me + 2 - 4 * y
    one = (1 - core) * along_x + core * along_y
    two = (1 - core) * along_y + core * along_x

    def copy_core(k):
        return pltpu.make_async_remote_copy(
            go.at[k % 2], r_core.at[k % SLOTS], core_send.at[k], core_recv.at[k], device_id={"dp": partner}, device_id_type=pl.DeviceIdType.MESH
        )

    def copy_first(k):
        return pltpu.make_async_remote_copy(
            first.at[k % 2], r_first.at[k % SLOTS], first_send.at[k], first_recv.at[k], device_id={"dp": one}, device_id_type=pl.DeviceIdType.MESH
        )

    def copy_second(k):
        return pltpu.make_async_remote_copy(
            second.at[k % 2], r_second.at[k % SLOTS], second_send.at[k], second_recv.at[k], device_id={"dp": two}, device_id_type=pl.DeviceIdType.MESH
        )

    @pl.when(j == 0)
    def _():
        barrier = pltpu.get_barrier_semaphore()
        for other in (partner, along_x, along_y):
            pl.semaphore_signal(barrier, inc=1, device_id={"dp": other}, device_id_type=pl.DeviceIdType.MESH)
        pl.semaphore_wait(barrier, 3)
        for r in range(8):
            c, u, v = r // 4, (r // 2) % 2, r % 2
            owner_core = (core + c) % 2
            du, dv = (1 - owner_core) * u + owner_core * v, (1 - owner_core) * v + owner_core * u
            owner = ((x + du) % 2) * 4 + ((y + dv) % 2) * 2 + owner_core
            columns = pl.ds(pl.multiple_of(owner * CHUNK, CHUNK), CHUNK)
            at[r * CHUNK : (r + 1) * CHUNK, :] = a_ref[:, columns].T
            dyt[r * CHUNK : (r + 1) * CHUNK, :] = dy_ref[:, columns].T

    def place(k, owner):
        return early_ref.at[owner, :, :, pl.ds(pl.multiple_of(k * BLOCK, BLOCK), BLOCK)]

    def keep(k):
        return pltpu.make_async_copy(own.at[k], place(k, me), sent.at[k, 7])

    def spread(k, way, source, owner, to):
        return pltpu.make_async_remote_copy(
            source, place(k, owner), sent.at[k, way], got.at[k, way], device_id={"dp": to}, device_id_type=pl.DeviceIdType.MESH
        )

    @pl.when(j >= STEPS)
    def _():
        k = j - STEPS
        copy_second(k).wait()
        s = k % SLOTS
        total = stay[s, 0].astype(F32) + r_core[s, 0].astype(F32) + r_first[s, 0].astype(F32) + r_second[s].astype(F32)
        if inner:

            @pl.when(k < SPLIT)
            def _():
                early_ref[...] = total.astype(BF16)

        @pl.when(k >= SPLIT)
        def _():
            out_ref[...] = total.astype(BF16)

        if not inner:

            @pl.when(k < SPLIT)
            def _():
                own[k] = total.astype(BF16)
                keep(k).start()
                for way, to in enumerate((two, one, partner)):
                    spread(k, way, own.at[k], me, to).start()

    if not inner:
        beyond = one + two - me

        @pl.when((j >= STEPS + LAG) & (j < STEPS + LAG + SPLIT))
        def _():
            k = j - STEPS - LAG
            spread(k, 0, own.at[k], me, two).wait_recv()
            spread(k, 3, place(k, two), two, one).start()
            spread(k, 4, place(k, two), two, partner).start()
            spread(k, 1, own.at[k], me, one).wait_recv()
            spread(k, 5, place(k, one), one, partner).start()

        @pl.when((j >= STEPS + 2 * LAG) & (j < STEPS + 2 * LAG + SPLIT))
        def _():
            k = j - STEPS - 2 * LAG
            spread(k, 3, place(k, two), two, one).wait_recv()
            spread(k, 6, place(k, beyond), beyond, partner).start()

        @pl.when((j >= STEPS + 3 * LAG) & (j < STEPS + 3 * LAG + SPLIT))
        def _():
            k = j - STEPS - 3 * LAG
            keep(k).wait()
            for way in range(7):
                spread(k, way, own.at[k], me, partner).wait_send()
            for way in (2, 4, 5, 6):
                spread(k, way, own.at[k], me, partner).wait_recv()

    @pl.when((j >= LAG + 1) & (j < units + LAG + 1))
    def _():
        k = j - LAG - 1
        copy_first(k).wait()
        s = k % SLOTS
        second[k % 2] = (stay[s, 1].astype(F32) + r_core[s, 1].astype(F32) + r_first[s, 1].astype(F32)).astype(BF16)
        copy_second(k).start()

    @pl.when((j >= 1) & (j < units + 1))
    def _():
        k = j - 1
        copy_core(k).wait()
        s = k % SLOTS
        first[k % 2] = (stay[s, 2:].astype(F32) + r_core[s, 2:].astype(F32)).astype(BF16)
        copy_first(k).start()

    def body(width):
        @pl.loop(0, TOKENS // ROWS)
        def _(i):
            rows = pl.ds(pl.multiple_of(i * ROWS, ROWS), ROWS)
            if inner:
                gate, up = gate_ref[rows, :width], up_ref[rows, :width]
            else:
                a = a_ref[rows, :]
                gate = dot(a, wg_ref[:, :width])
                up = dot(a, wu_ref[:, :width])
            by_act = dot_nt(dy_ref[rows, :], wd_ref[:width, :]).astype(BF16).astype(F32)
            sig = jax.nn.sigmoid(gate)
            silu = gate * sig
            act_s[rows, :width] = (silu * up).astype(BF16)
            du = (by_act * silu).astype(BF16)
            dg = (by_act * up * (sig + silu * (1.0 - sig))).astype(BF16)
            dgu_s[rows, :width] = dg
            dgu_s[rows, width : 2 * width] = du
            if not inner:
                dg_out[rows, :width] = dg
                du_out[rows, :width] = du

        def gradients(c, into):
            half = pl.ds(c * 4 * CHUNK, 4 * CHUNK)
            term = dot(at[half, :], dgu_s[:, : 2 * width]).astype(BF16)
            into[:, 0, :, :width] = term[:, :width].reshape(4, CHUNK, width)
            into[:, 1, :, :width] = term[:, width:].reshape(4, CHUNK, width)
            into[:, 2, :, :width] = dot(dyt[half, :], act_s[:, :width]).astype(BF16).reshape(4, CHUNK, width)

        gradients(1, go.at[j % 2])
        copy_core(j).start()
        gradients(0, stay.at[j % SLOTS])

    by_width(j, units, last, body)


def backward(layer, inner, collective_id, a, dy, wd, left, right):
    units = pl.cdiv(FF, BLOCK)
    last = FF - (units - 1) * BLOCK
    size, early = FF, SPLIT * BLOCK
    assert units >= SPLIT + LAG + 1
    whole = lambda j: (0, 0)
    unit = lambda j: jnp.minimum(j, units - 1)
    in_specs = [once((TOKENS, D), whole), once((TOKENS, D), whole), pl.BlockSpec((None, BLOCK, D), lambda j: (layer, unit(j), 0))]
    if inner:
        in_specs += [pl.BlockSpec((TOKENS, BLOCK), lambda j: (0, unit(j)))] * 2
        out_specs = [pl.BlockSpec((3, CHUNK, BLOCK), lambda j: (0, 0, jnp.clip(j - STEPS, 0, SPLIT - 1)))]
        out_shape = [jax.ShapeDtypeStruct((3, CHUNK, early), BF16)]
    else:
        in_specs += [pl.BlockSpec((None, D, BLOCK), lambda j: (layer, 0, unit(j)))] * 2
        out_specs = [pl.BlockSpec(memory_space=pl.ANY)]
        out_shape = [jax.ShapeDtypeStruct((8, 3, CHUNK, early), BF16)]
    out_specs.append(pl.BlockSpec((3, CHUNK, BLOCK), lambda j: (0, 0, jnp.clip(j - STEPS - SPLIT, 0, units - SPLIT - 1))))
    out_shape.append(jax.ShapeDtypeStruct((3, CHUNK, FF - early), BF16))
    scratch = [
        pltpu.VMEM((D, TOKENS), BF16),
        pltpu.VMEM((D, TOKENS), BF16),
        pltpu.VMEM((TOKENS, BLOCK), BF16),
        pltpu.VMEM((TOKENS, 2 * BLOCK), BF16),
        pltpu.VMEM((SLOTS, 4, 3, CHUNK, BLOCK), BF16),
        pltpu.VMEM((2, 4, 3, CHUNK, BLOCK), BF16),
        pltpu.VMEM((2, 2, 3, CHUNK, BLOCK), BF16),
        pltpu.VMEM((2, 3, CHUNK, BLOCK), BF16),
        pltpu.VMEM((SLOTS, 4, 3, CHUNK, BLOCK), BF16),
        pltpu.VMEM((SLOTS, 2, 3, CHUNK, BLOCK), BF16),
        pltpu.VMEM((SLOTS, 3, CHUNK, BLOCK), BF16),
    ] + [pltpu.SemaphoreType.DMA((units,))] * 6
    if not inner:
        out_specs += [pl.BlockSpec((TOKENS, BLOCK), lambda j: (0, unit(j)))] * 2
        out_shape += [jax.ShapeDtypeStruct((TOKENS, size), BF16)] * 2
        scratch += [pltpu.VMEM((SPLIT, 3, CHUNK, BLOCK), BF16), pltpu.SemaphoreType.DMA((SPLIT, 8)), pltpu.SemaphoreType.DMA((SPLIT, 7))]
    return pl.pallas_call(
        functools.partial(backward_kernel, units, last, inner),
        grid=(units + STEPS,),
        in_specs=in_specs,
        out_specs=out_specs,
        out_shape=out_shape,
        scratch_shapes=scratch,
        compiler_params=pltpu.CompilerParams(vmem_limit_bytes=VMEM, collective_id=collective_id, has_side_effects=True),
        cost_estimate=pl.CostEstimate(flops=(8 if inner else 12) * TOKENS * D * size, bytes_accessed=40_000_000, transcendentals=TOKENS * size),
        name=f"backward{layer}",
    )(a, dy, wd, left, right)


def input_kernel(dg_ref, du_ref, wg_ref, wu_ref, h_ref, dy_ref, g_ref, *refs):
    out_ref = refs[9]
    da = dot_nt(dg_ref[...], wg_ref[...]) + dot_nt(du_ref[...], wu_ref[...])
    h, d = h_ref[...].astype(F32), da.astype(BF16).astype(F32)
    scale = rms(h)
    dh = d * scale - h * (scale**3 / D) * jnp.sum(d * h, -1, keepdims=True)
    out_ref[...] = (dy_ref[...].astype(F32) + dh.astype(BF16).astype(F32)).astype(BF16)
    adamw_kernel(g_ref, *refs[:9], *refs[10:])


def by_input(layer, dg, du, wg, wu, h, dy, g, arrays):
    rows = TOKENS // 8
    weight = once((None, D, FF), lambda i: (layer, 0, 0))
    state = pl.BlockSpec((rows, D), lambda i: (i, 0))
    more_in, more_out, more_shape = adamw_specs(layer, 0, SPLIT * BLOCK, SPLIT * BLOCK, arrays)
    elements = 3 * D * SPLIT * BLOCK
    return pl.pallas_call(
        input_kernel,
        grid=(8,),
        in_specs=[pl.BlockSpec((rows, FF), lambda i: (i, 0))] * 2 + [weight, weight, state, state] + more_in,
        out_specs=[state] + more_out,
        out_shape=[jax.ShapeDtypeStruct((TOKENS, D), BF16)] + more_shape,
        compiler_params=pltpu.CompilerParams(vmem_limit_bytes=VMEM),
        cost_estimate=pl.CostEstimate(flops=4 * TOKENS * D * FF, bytes_accessed=50_000_000 + 22 * elements, transcendentals=TOKENS + elements),
        name="by_input",
    )(dg, du, wg, wu, h, dy, g, *arrays)


WIDE = 640


def adamw_kernel(g_ref, *refs):
    ins, outs = refs[:9], refs[-9:]
    for which in range(3):
        g = g_ref[which].astype(F32)
        if which == 2:
            g = g.T
        w, m, v = (ins[3 * kind + which][...].astype(F32) for kind in range(3))
        m = 0.9 * m + 0.1 * g
        v = 0.95 * v + 0.05 * g * g
        step = m * lax.rsqrt(v + 1e-8) + 0.1 * w
        outs[which][...] = (w - 0.02 * step).astype(BF16)
        outs[3 + which][...] = m
        outs[6 + which][...] = v


def adamw_specs(layer, first, size, wide, arrays):
    start, across = first // wide, size // wide
    row = pl.BlockSpec((None, CHUNK, wide), lambda t: (layer, t // across, start + t % across))
    column = pl.BlockSpec((None, wide, CHUNK), lambda t: (layer, start + t % across, t // across))
    nine = [row, row, column] * 3
    types = [BF16] * 3 + [F32] * 6
    gradient = pl.BlockSpec((None, 3, CHUNK, wide), lambda t: (t // across, 0, 0, t % across))
    return [gradient] + nine, nine, [jax.ShapeDtypeStruct(a.shape, t) for a, t in zip(arrays, types)]


def adamw(layer, first, size, g, arrays, so_far):
    in_specs, out_specs, out_shape = adamw_specs(layer, first, size, WIDE, arrays)
    elements = 3 * D * size
    return pl.pallas_call(
        adamw_kernel,
        grid=(8 * size // WIDE,),
        in_specs=in_specs + [pl.BlockSpec(memory_space=pl.ANY)] * 9,
        out_specs=out_specs,
        out_shape=out_shape,
        input_output_aliases={10 + i: i for i in range(9)},
        compiler_params=pltpu.CompilerParams(vmem_limit_bytes=VMEM),
        cost_estimate=pl.CostEstimate(flops=40 * elements, bytes_accessed=22 * elements, transcendentals=elements),
        name=f"adamw{layer}_{first}",
    )(g, *arrays, *so_far)


def solution(mesh):
    def step(x, dy, *arrays):
        wg, wu, wd = arrays[:3]
        x, dy = x[0], dy[0]
        early = SPLIT * BLOCK
        gate, up, a0, h1, a1 = forward(x, wg, wu, wd)
        all1, own1, dg, du = backward(1, False, 0, a1, dy, wd, wg, wu)
        rest1 = lax.all_gather(own1, "dp")
        dh1, *outs = by_input(1, dg, du, wg, wu, h1, dy, all1, arrays)
        first0, own0 = backward(0, True, 1, a0, dh1, wd, gate, up)
        rest0 = lax.all_gather(own0, "dp")
        first0, _ = lax.optimization_barrier((first0, own0))
        first0 = lax.all_gather(first0, "dp")
        outs = adamw(1, early, FF - early, rest1, arrays, outs)
        outs = adamw(0, early, FF - early, rest0, arrays, outs)
        return tuple(adamw(0, 0, early, first0, arrays, outs))

    return jax.shard_map(
        step,
        mesh=mesh,
        in_specs=(P(("rep", "dp"), None, None),) * 2 + (P(None, None, None),) * 9,
        out_specs=(P("rep", None, None),) * 9,
        check_vma=False,
    )
```
